256 devices in a mesh: patch: 128 (over z, y, x), grp: 2 (over core).
Axes of the slice: x: 4, y: 4, z: 8, core: 2. Of those that a mesh axis runs over, the one named last changes fastest.
Arguments:
- node_latent: float32 [40960, 512], P(('patch', 'grp')), may hold values from -6 to 6
- edge_latent: float32 [262144, 512], P(('patch', 'grp')), may hold values from -6 to 6
- node_cot: float32 [40960, 512], P(('patch', 'grp')), may hold values from -6 to 6
- edge_cot: float32 [262144, 512], P(('patch', 'grp')), may hold values from -6 to 6
- edge_w1: bfloat16 [1536, 512], replicated, may hold values from -0.15625 to 0.15625
- edge_w2: bfloat16 [512, 512], replicated, may hold values from -0.25 to 0.25
- edge_gain: float32 [512], replicated, may hold values from 0.1 to 1.9
- node_w1: bfloat16 [1024, 512], replicated, may hold values from -0.1875 to 0.1875
- node_w2: bfloat16 [512, 512], replicated, may hold values from -0.25 to 0.25
- node_gain: float32 [512], replicated, may hold values from 0.1 to 1.9
- senders: int32 [262144], P(('patch', 'grp')), may hold values from 0 to 959, as said below
- receivers: int32 [262144], P(('patch', 'grp')), may hold values from 0 to 319
- counts: int32 [256], P(('patch', 'grp')), may hold values from 256 to 1024, as said below
Outputs:
- node_grad: float32 [40960, 512], P(('patch', 'grp'))
- edge_grad: float32 [262144, 512], P(('patch', 'grp'))
- grad_edge_w1: float32 [1536, 512], P('grp')
- grad_edge_w2: float32 [512, 512], P('grp')
- grad_node_w1: float32 [1024, 512], P('grp')
- grad_node_w2: float32 [512, 512], P('grp')
The draws below stay inside these ranges and needn't reach their ends.
Inputs may be any that keep to these rules, and one draw needn't show every extreme that they name: `senders`: indices into the nodes of the previous patch, the own patch and the next patch (patches taken cyclically), 320 rows each, in that order. `counts`: each device's live edges fill its first slots; some device is full in every draw.
All inputs are finite; a program needn't handle non-finite values.
Results may differ from the reference program's by a relative error of at most 0.0068.
Values may be sent and summed in bfloat16 or wider, within the bound.
No kernel may reach another device: no remote copies, remote signals or barrier semaphores. Data moves between devices by JAX's collectives and lax.ppermute only.
A program may use at most 128 MiB of HBM per device.

```python
import math
import jax
import jax.numpy as jnp
import numpy as np
from jax import lax

D = 512
EDGE_DEV = 1024
NODE_PATCH = 320
NODES = 40960
EDGES = 262144
N_PATCH = 128
N_GRP = 2
DEVICES = 256


def draw_senders(key, part):
    first, second = jax.random.split(jax.random.fold_in(key, 11))
    pick = jax.random.randint(first, (EDGES,), 0, 5)
    slab = jnp.where(pick == 0, 0, jnp.where(pick == 4, 2, 1))
    within = jax.random.randint(second, (EDGES,), 0, NODE_PATCH)
    return (slab * NODE_PATCH + within).astype(jnp.int32)


def draw_counts(key, part):
    first, second = jax.random.split(jax.random.fold_in(key, 23))
    level = jax.random.randint(first, (DEVICES,), 0, 65)
    base = EDGE_DEV // 4 + 3 * EDGE_DEV // 4 * level * level // 4096
    full = jax.random.randint(second, (), 0, DEVICES)
    return jnp.where(jnp.arange(DEVICES) == full, EDGE_DEV, base).astype(jnp.int32)


def touch_ends(drawn, rng, least, top_value):
    longest = drawn.shape.index(max(drawn.shape))
    spots = []
    for shift in (0, 1):
        where = [jax.random.randint(jax.random.fold_in(rng, axis), (), 0, length) for axis, length in enumerate(drawn.shape)]
        where[longest] = (where[longest] + shift) % drawn.shape[longest]
        spots.append(tuple(where))
    return drawn.at[spots[0]].set(least).at[spots[1]].set(top_value)


def steps_of(own_key, dims, cuts, smallest, largest):
    level = 1.0
    for axis_at, shards_of in cuts:
        heights = jax.random.uniform(jax.random.fold_in(jax.random.fold_in(own_key, 6), axis_at), (shards_of,), jnp.float32, smallest / len(cuts), largest / len(cuts))
        level = level * jnp.repeat(jnp.exp(heights), dims[axis_at] // shards_of).reshape((-1,) + (1,) * (len(dims) - 1 - axis_at))
    return level


def rank_table(number_of, skew):
    weights = [(1 << 20) // math.isqrt(standing ** skew) + 1 for standing in range(1, number_of + 1)]
    deviation = 1 + sum(weights) // (1 << 30)
    return np.cumsum(np.array([max(1, weight // deviation) for weight in weights]))


def ranked(rng, dims, amount, slope):
    grid = rank_table(amount, slope)
    lot = jax.random.randint(jax.random.fold_in(rng, 1), dims, 0, int(grid[amount - 1]))
    grade = jnp.searchsorted(jnp.asarray(grid, jnp.int32), lot, side="right")
    return jax.random.permutation(jax.random.fold_in(rng, 2), amount)[grade].astype(jnp.int32)


def noise(key, extent, width, limit, cuts=(), held_as=jnp.bfloat16):
    array = width * jax.random.normal(key, extent, jnp.float32)
    if cuts:
        array = array * steps_of(key, extent, cuts, -0.22, 0.18)
    return jnp.clip(array, -limit, limit).astype(held_as)


def setup_inputs(seed: int = 0) -> dict:
    keys = jax.random.split(jax.random.key(seed), 14)
    return {
        "node_latent": noise(keys[0], (NODES, D), 1.0, 6.0, ((0, 256),), jnp.float32),
        "edge_latent": noise(keys[1], (EDGES, D), 1.0, 6.0, ((0, 256),), jnp.float32),
        "node_cot": noise(keys[2], (NODES, D), 1.0, 6.0, ((0, 256),), jnp.float32),
        "edge_cot": noise(keys[3], (EDGES, D), 1.0, 6.0, ((0, 256),), jnp.float32),
        "edge_w1": noise(keys[4], (3 * D, D), (3 * D) ** -0.5, 0.15625),
        "edge_w2": noise(keys[5], (D, D), D ** -0.5, 0.25),
        "edge_gain": jnp.clip(1.0 + 0.18 * jax.random.normal(keys[6], (D,), jnp.float32), 0.1, 1.9),
        "node_w1": noise(keys[7], (2 * D, D), (2 * D) ** -0.5, 0.1875),
        "node_w2": noise(keys[8], (D, D), D ** -0.5, 0.25),
        "node_gain": jnp.clip(1.0 + 0.18 * jax.random.normal(keys[9], (D,), jnp.float32), 0.1, 1.9),
        "senders": draw_senders(jax.random.fold_in(keys[13], 71), 0),
        "receivers": touch_ends(ranked(keys[11], (EDGES,), NODE_PATCH, 1), jax.random.fold_in(keys[11], 3), 0, NODE_PATCH - 1).astype(jnp.int32),
        "counts": draw_counts(jax.random.fold_in(keys[13], 71), 0),
    }


EPS = 1e-05

def silu_grad(pre):
    sig = jax.nn.sigmoid(pre)
    return sig * (1.0 + pre * (1.0 - sig))

def norm_forward(out, gain):
    center = out - lax.optimization_barrier(jnp.mean(out, axis=-1, keepdims=True))
    inv_std = lax.rsqrt(lax.optimization_barrier(jnp.mean(center * center, axis=-1, keepdims=True)) + EPS)
    normed = center * inv_std
    return (normed * gain, normed, inv_std)

def norm_backward(grad_y, gain, normed, inv_std):
    scaled = grad_y * gain
    return inv_std * (scaled - lax.optimization_barrier(jnp.mean(scaled, axis=-1, keepdims=True)) - normed * lax.optimization_barrier(jnp.mean(scaled * normed, axis=-1, keepdims=True)))

def mlp_forward(inputs, first, second, gain):
    pre = jnp.dot(inputs, first, preferred_element_type=jnp.float32)
    act = jax.nn.silu(pre).astype(jnp.bfloat16)
    out = jnp.dot(act, second, preferred_element_type=jnp.float32)
    upd, normed, inv_std = norm_forward(out, gain)
    return (upd, pre, act, normed, inv_std)

def mlp_backward(grad_y, inputs, first, second, gain, pre, act, normed, inv_std):
    grad_out = norm_backward(grad_y, gain, normed, inv_std).astype(jnp.bfloat16)
    grad_second = jnp.dot(act.T, grad_out, preferred_element_type=jnp.float32)
    grad_act = jnp.dot(grad_out, second.T, preferred_element_type=jnp.float32)
    grad_pre = (grad_act * silu_grad(pre)).astype(jnp.bfloat16)
    grad_first = jnp.dot(inputs.T, grad_pre, preferred_element_type=jnp.float32)
    grad_in = jnp.dot(grad_pre, first.T, preferred_element_type=jnp.float32)
    return (grad_in, grad_first, grad_second)

def reference(node_latent, edge_latent, node_cot, edge_cot, edge_w1, edge_w2, edge_gain, node_w1, node_w2, node_gain, senders, receivers, counts):
    slots = jnp.arange(EDGES, dtype=jnp.int32)
    device = slots // EDGE_DEV
    patch_of = device // N_GRP
    live = (slots % EDGE_DEV < counts[device]).astype(jnp.float32)[:, None]
    recv_node = (patch_of * NODE_PATCH + receivers).astype(jnp.int32)
    slab = senders // NODE_PATCH
    send_node = ((patch_of + slab - 1) % N_PATCH * NODE_PATCH + senders % NODE_PATCH).astype(jnp.int32)
    node_bf = node_latent.astype(jnp.bfloat16)
    edge_in = jnp.concatenate([edge_latent.astype(jnp.bfloat16), node_bf[send_node], node_bf[recv_node]], axis=1)
    edge_upd, edge_pre, edge_act, edge_normed, edge_inv = mlp_forward(edge_in, edge_w1, edge_w2, edge_gain)
    edge_upd = edge_upd * live
    aggregate = jax.ops.segment_sum(edge_upd, recv_node, num_segments=NODES)
    node_in = jnp.concatenate([node_bf, aggregate.astype(jnp.bfloat16)], axis=1)
    node_upd, node_pre, node_act, node_normed, node_inv = mlp_forward(node_in, node_w1, node_w2, node_gain)
    node_gin, grad_node_w1, grad_node_w2 = mlp_backward(node_cot, node_in, node_w1, node_w2, node_gain, node_pre, node_act, node_normed, node_inv)
    grad_agg = node_gin[:, D:]
    edge_gupd = (edge_cot + grad_agg[recv_node]) * live
    edge_gin, grad_edge_w1, grad_edge_w2 = mlp_backward(edge_gupd, edge_in, edge_w1, edge_w2, edge_gain, edge_pre, edge_act, edge_normed, edge_inv)
    edge_grad = edge_cot + edge_gin[:, :D]
    node_grad = node_cot + node_gin[:, :D]
    node_grad = node_grad + jax.ops.segment_sum(edge_gin[:, D:2 * D], send_node, num_segments=NODES)
    node_grad = node_grad + jax.ops.segment_sum(edge_gin[:, 2 * D:], recv_node, num_segments=NODES)
    return (node_grad, edge_grad, grad_edge_w1, grad_edge_w2, grad_node_w1, grad_node_w2)
```

```python
import functools
import numpy as np
import jax
import jax.numpy as jnp
from jax import lax
from jax.experimental import pallas as pl
from jax.experimental.pallas import tpu as pltpu
from jax.sharding import PartitionSpec as P

EPS = 1e-05
F32 = jnp.float32
BF = jnp.bfloat16
TILE = 256


def mm(a, b):
    return jnp.dot(a, b, preferred_element_type=F32)


def mm_nt(a, b):
    return lax.dot_general(a, b, (((1,), (1,)), ((), ())), preferred_element_type=F32)


def mm_tn(a, b):
    return lax.dot_general(a, b, (((0,), (0,)), ((), ())), preferred_element_type=F32)


def split(x):
    high = x.astype(BF)
    return high, (x - high.astype(F32)).astype(BF)


def hot_rows(index, rows):
    grid = lax.broadcasted_iota(jnp.int32, (rows, index.shape[1]), 0)
    return jnp.where(grid == index, 1.0, 0.0).astype(BF)


def hot_cols(index, cols):
    grid = lax.broadcasted_iota(jnp.int32, (index.shape[0], cols), 1)
    return jnp.where(grid == index, 1.0, 0.0).astype(BF)


def sigmoid(x):
    return 1.0 / (1.0 + jnp.exp(-x))


def norm_forward(out):
    center = out - jnp.mean(out, axis=-1, keepdims=True)
    inv_std = lax.rsqrt(jnp.mean(center * center, axis=-1, keepdims=True) + EPS)
    return center * inv_std, inv_std


def norm_backward(grad_y, gain, normed, inv_std):
    scaled = grad_y * gain
    return inv_std * (
        scaled
        - jnp.mean(scaled, axis=-1, keepdims=True)
        - normed * jnp.mean(scaled * normed, axis=-1, keepdims=True)
    )


def alive(cnt_ref, step, tile):
    slot = step * tile + lax.broadcasted_iota(jnp.int32, (tile, 1), 0)
    return jnp.where(slot < cnt_ref[0], 1.0, 0.0)


def edge_forward(
    cnt_ref, lat_ref, near_ref, far_ref, sc_ref, rc_ref, rr_ref, w1_ref, w2_ref, gain_ref,
    ein_ref, pre_ref, out_ref, agg_ref, ext, own,
):
    step = pl.program_id(0)
    tile, width = lat_ref.shape
    half = near_ref.shape[0]
    rows = half // 3

    @pl.when(step == 0)
    def _():
        ext[:half] = near_ref[...]
        ext[half:] = far_ref[...]
        own[:rows] = near_ref[rows : 2 * rows]
        own[rows:] = far_ref[rows : 2 * rows]
        agg_ref[...] = jnp.zeros_like(agg_ref)

    ein_ref[:, :width] = lat_ref[...].astype(BF)
    ein_ref[:, width : 2 * width] = mm(hot_cols(sc_ref[...], 2 * half), ext[...]).astype(BF)
    ein_ref[:, 2 * width :] = mm(hot_cols(rc_ref[...], 2 * rows), own[...]).astype(BF)
    pre = mm(ein_ref[...], w1_ref[...])
    pre_ref[...] = pre
    out = mm((pre * sigmoid(pre)).astype(BF), w2_ref[...])
    out_ref[...] = out
    normed, _ = norm_forward(out)
    upd = normed * gain_ref[...] * alive(cnt_ref, step, tile)
    high, low = split(upd)
    hot = hot_rows(rr_ref[...], 2 * rows)
    agg_ref[...] += mm(hot, high) + mm(hot, low)


def node_both(
    g_ref, near_ref, far_ref, agg_ref, got_ref, cot_ref, cot_far_ref, w1_ref, w2_ref, gain_ref,
    gin_ref, gagg_ref, gw_ref, acts,
):
    rows = cot_ref.shape[0]
    width = cot_ref.shape[1]
    g = g_ref[0]
    nodes = jnp.concatenate([near_ref[rows : 2 * rows], far_ref[rows : 2 * rows]], axis=0)
    agg = jnp.concatenate(
        [agg_ref[:rows] + got_ref[rows:], agg_ref[rows:] + got_ref[:rows]], axis=0
    ).astype(BF)
    cot = jnp.concatenate([cot_ref[...], cot_far_ref[...]], axis=0)
    pre = mm(nodes, w1_ref[:width]) + mm(agg, w1_ref[width:])
    sig = sigmoid(pre)
    act = (pre * sig).astype(BF)
    acts[...] = act
    normed, inv_std = norm_forward(mm(act, w2_ref[...]))
    gout = norm_backward(cot, gain_ref[...], normed, inv_std).astype(BF)
    gpre = (mm_nt(gout, w2_ref[...]) * (sig * (1.0 + pre * (1.0 - sig)))).astype(BF)
    gin_ref[...] = cot_ref[...] + mm_nt(gpre[:rows], w1_ref[:width])
    gagg_ref[...] = mm_nt(gpre, w1_ref[width:])
    part = jnp.where(g == 0, nodes.astype(F32), agg.astype(F32)).astype(BF)
    gw_ref[:width] = mm_tn(part, gpre).astype(BF)
    some = acts[:, pl.ds(pl.multiple_of(g * (width // 2), 128), width // 2)]
    gw_ref[width:] = mm_tn(some, gout).astype(BF)


def edge_backward(
    cnt_ref, g_ref, cot_ref, gagg_ref, rc_ref, pre_ref, out_ref, ein_ref, w2_ref, gain_ref,
    gpre_ref, mine_ref, theirs_ref, high, low, acts, gouts,
):
    step = pl.program_id(0)
    tile, width = cot_ref.shape

    @pl.when(step == 0)
    def _():
        a, b = split(gagg_ref[...])
        high[...] = a
        low[...] = b

    hot = hot_cols(rc_ref[...], gagg_ref.shape[0])
    grad = cot_ref[...] + (mm(hot, high[...]) + mm(hot, low[...]))
    grad = grad * alive(cnt_ref, step, tile)
    normed, inv_std = norm_forward(out_ref[...])
    gout = norm_backward(grad, gain_ref[...], normed, inv_std).astype(BF)
    pre = pre_ref[...]
    sig = sigmoid(pre)
    here = pl.ds(pl.multiple_of(step * tile, tile), tile)
    acts[here] = (pre * sig).astype(BF)
    gouts[here] = gout
    gpre_ref[here] = (mm_nt(gout, w2_ref[...]) * (sig * (1.0 + pre * (1.0 - sig)))).astype(BF)

    @pl.when(step == pl.num_programs(0) - 1)
    def _():
        big, small = 3 * width // 2, width // 2
        for k in range(2):
            side = g_ref[0] if k == 1 else 1 - g_ref[0]
            cols = ein_ref[:, pl.ds(pl.multiple_of(side * big, 128), big)]
            some = acts[:, pl.ds(pl.multiple_of(side * small, 128), small)]
            first = mm_tn(cols, gpre_ref[...])
            second = mm_tn(some, gouts[...])
            dst = mine_ref if k == 1 else theirs_ref
            dst[:big] = first.astype(dst.dtype)
            dst[big:] = second.astype(dst.dtype)


def edge_inputs(
    gpre_ref, cot_ref, sr_ref, rr_ref, w1_ref, grad_ref, mine_ref, theirs_ref, sent, recvd,
):
    step = pl.program_id(0)
    width = cot_ref.shape[1]
    half, rows = sent.shape[0] // 2, recvd.shape[0] // 2

    @pl.when(step == 0)
    def _():
        sent[...] = jnp.zeros_like(sent)
        recvd[...] = jnp.zeros_like(recvd)

    gpre = gpre_ref[...]
    grad_ref[...] = cot_ref[...] + mm_nt(gpre, w1_ref[...])
    sent[...] += mm(hot_rows(sr_ref[...], 2 * half), gpre)
    recvd[...] += mm(hot_rows(rr_ref[...], 2 * rows), gpre)

    @pl.when(step == pl.num_programs(0) - 1)
    def _():
        mine_ref[:half] = sent[:half]
        mine_ref[half:] = recvd[:rows]
        theirs_ref[:half] = sent[half:].astype(BF)
        theirs_ref[half:] = recvd[rows:].astype(BF)


def whole(shape):
    return pl.BlockSpec(shape, lambda i: (0,) * len(shape))


def rows_of(tile, width):
    return pl.BlockSpec((tile, width), lambda i: (i, 0))


def cols_of(tile):
    return pl.BlockSpec((1, tile), lambda i: (0, i))


SMEM = pl.BlockSpec(memory_space=pltpu.SMEM)


def call(body, grid, ins, outs, shapes, scratch, name, flops, traffic, limit):
    return pl.pallas_call(
        body,
        grid=(grid,),
        in_specs=ins,
        out_specs=outs,
        out_shape=[jax.ShapeDtypeStruct(s, d) for s, d in shapes],
        scratch_shapes=[pltpu.VMEM(s, d) for s, d in scratch],
        name=name,
        cost_estimate=pl.CostEstimate(flops=flops, bytes_accessed=traffic, transcendentals=0),
        compiler_params=pltpu.CompilerParams(
            dimension_semantics=("arbitrary",), vmem_limit_bytes=limit << 20
        ),
    )


def node_finish(mine_ref, got_ref, next_ref, prev_ref, gin_ref, w1_ref, out_ref):
    rows, width = gin_ref.shape
    mid = slice(rows, 2 * rows)
    sent = mine_ref[mid] + got_ref[mid].astype(F32)
    sent = (sent + next_ref[...].astype(F32) + prev_ref[...].astype(F32)).astype(BF)
    recvd = (mine_ref[3 * rows :] + got_ref[3 * rows :].astype(F32)).astype(BF)
    out_ref[...] = (
        gin_ref[...]
        + mm_nt(sent, w1_ref[width : 2 * width])
        + mm_nt(recvd, w1_ref[2 * width :])
    )


def take(x, start, size, dim=0):
    return lax.dynamic_slice_in_dim(x, start, size, dim)


class Torus:
    def __init__(self, sizes):
        self.sizes = sizes
        self.count = int(np.prod(sizes))
        where = lax.axis_index("patch")
        here = []
        for size in reversed(sizes):
            here.append(lax.rem(where, size))
            where = lax.div(where, size)
        self.here = here[::-1]

    def pairs(self, move):
        out = []
        for source in range(self.count):
            at = list(np.unravel_index(source, self.sizes))
            out.append((source, int(np.ravel_multi_index(move(at), self.sizes))))
        return out

    def shift(self, value, axis, steps):
        def move(at):
            at[axis] = (at[axis] + steps) % self.sizes[axis]
            return at

        return lax.ppermute(value, "patch", self.pairs(move))

    def swap(self, value, axis, bit):
        def move(at):
            at[axis] = at[axis] ^ bit
            return at

        return lax.ppermute(value, "patch", self.pairs(move))

    def steps(self, axis):
        size = self.sizes[axis]
        order = [s for k in range(1, size // 2 + 1) for s in (k, -k)]
        return order[: size - 1]

    def scatter_sum(self, value, axis):
        size = self.sizes[axis]
        rows = value.shape[0] // size
        at = self.here[axis]
        got = [
            self.shift(take(value, lax.rem(at + s + size, size) * rows, rows), axis, s)
            for s in self.steps(axis)
        ]
        total = take(value, at * rows, rows).astype(F32)
        for part in got:
            total = total + part.astype(F32)
        return total

    def gather(self, value, axis):
        size = self.sizes[axis]
        rows = value.shape[0]
        at = self.here[axis]
        whole_value = jnp.zeros((rows * size, value.shape[1]), value.dtype)
        whole_value = lax.dynamic_update_slice_in_dim(whole_value, value, at * rows, 0)
        for s in self.steps(axis):
            slot = lax.rem(at - s + size, size)
            whole_value = lax.dynamic_update_slice_in_dim(
                whole_value, self.shift(value, axis, s), slot * rows, 0
            )
        return whole_value

    def halve(self, value, axis, bit, dim):
        size = value.shape[dim] // 2
        side = lax.rem(lax.div(self.here[axis], bit), 2)
        got = self.swap(take(value, (1 - side) * size, size, dim), axis, bit)
        return take(value, side * size, size, dim) + got

    def double(self, value, axis, bit, dim):
        side = lax.rem(lax.div(self.here[axis], bit), 2)
        got = self.swap(value, axis, bit)
        low = jnp.where(side == 0, value, got)
        high = jnp.where(side == 0, got, value)
        return jnp.concatenate([low, high], axis=dim)


def sum_over_patches(first, second, torus):
    z, y, x = 0, 1, 2
    a = torus.scatter_sum(first, x)
    b = torus.scatter_sum(second, y)
    a = torus.scatter_sum(a.astype(BF), y)
    b = torus.scatter_sum(b.astype(BF), x)
    part = jnp.concatenate([a, b], axis=0)
    dims = {1: 0, 2: 1, 4: 1}
    for bit, dim in dims.items():
        part = torus.halve(part, z, bit, dim)
    part = part.astype(BF)
    for bit, dim in reversed(dims.items()):
        part = torus.double(part, z, bit, dim)
    rows = part.shape[0] // 2
    a = torus.gather(torus.gather(part[:rows], y), x)
    b = torus.gather(torus.gather(part[rows:], x), y)
    return a, b


def local(
    node_latent, edge_latent, node_cot, edge_cot, edge_w1, edge_w2, edge_gain,
    node_w1, node_w2, node_gain, senders, receivers, counts,
):
    rows, width = node_latent.shape
    edges = edge_latent.shape[0]
    tiles = edges // TILE
    n_patch = lax.axis_size("patch")
    torus = Torus((8, 4, n_patch // 32))
    g = lax.axis_index("grp").astype(jnp.int32)
    other = [(0, 1), (1, 0)]
    up = [(i, (i + 1) % n_patch) for i in range(n_patch)]
    down = [(j, i) for i, j in up]

    node_bf = node_latent.astype(BF)
    before = lax.ppermute(node_bf, "patch", up)
    after = lax.ppermute(node_bf, "patch", down)
    near = jnp.concatenate([before, node_bf, after], axis=0)
    far = lax.ppermute(near, "grp", other)
    cot_far = lax.ppermute(node_cot, "grp", other)

    slab, place = senders // (2 * rows), senders % (2 * rows)
    side = jnp.where(place // rows == g, 0, 3 * rows)
    send_at = side + slab * rows + place % rows
    recv_at = jnp.where(receivers // rows == g, 0, rows) + receivers % rows
    send_col, send_row = send_at[:, None], send_at[None, :]
    recv_col, recv_row = recv_at[:, None], recv_at[None, :]
    egain, ngain = edge_gain[None, :], node_gain[None, :]
    which = g[None]

    sq = edges * width * width
    edge_in, edge_pre, edge_out, agg = call(
        edge_forward, tiles,
        [SMEM, rows_of(TILE, width), whole((3 * rows, width)), whole((3 * rows, width)),
         rows_of(TILE, 1), rows_of(TILE, 1), cols_of(TILE),
         whole((3 * width, width)), whole((width, width)), whole((1, width))],
        [rows_of(TILE, 3 * width), rows_of(TILE, width), rows_of(TILE, width), whole((2 * rows, width))],
        [((edges, 3 * width), BF), ((edges, width), F32), ((edges, width), F32), ((2 * rows, width), F32)],
        [((6 * rows, width), BF), ((2 * rows, width), BF)],
        "edge_forward", 14 * sq, 12 << 20, 40,
    )(counts, edge_latent, near, far, send_col, recv_col, recv_row, edge_w1, edge_w2, egain)

    agg_far = lax.ppermute(agg, "grp", other)
    node_gin, gagg, node_gw = call(
        node_both, 1,
        [SMEM, whole((3 * rows, width)), whole((3 * rows, width)), whole((2 * rows, width)),
         whole((2 * rows, width)), whole((rows, width)), whole((rows, width)),
         whole((2 * width, width)), whole((width, width)), whole((1, width))],
        [whole((rows, width)), whole((2 * rows, width)), whole((3 * width // 2, width))],
        [((rows, width), F32), ((2 * rows, width), F32), ((3 * width // 2, width), BF)],
        [((2 * rows, width), BF)],
        "node_both", 5 * sq, 6 << 20, 40,
    )(which, near, far, agg, agg_far, node_cot, cot_far, node_w1, node_w2, ngain)

    gpre, gw_mine, gw_theirs = call(
        edge_backward, tiles,
        [SMEM, SMEM, rows_of(TILE, width), whole((2 * rows, width)), rows_of(TILE, 1),
         rows_of(TILE, width), rows_of(TILE, width), whole((edges, 3 * width)),
         whole((width, width)), whole((1, width))],
        [whole((edges, width)), whole((2 * width, width)), whole((2 * width, width))],
        [((edges, width), BF), ((2 * width, width), F32), ((2 * width, width), BF)],
        [((2 * rows, width), BF), ((2 * rows, width), BF), ((edges, width), BF), ((edges, width), BF)],
        "edge_backward", 12 * sq, 14 << 20, 48,
    )(counts, which, edge_cot, gagg, recv_col, edge_pre, edge_out, edge_in, edge_w2, egain)

    gw_far = lax.ppermute(gw_theirs, "grp", other)
    gw = (gw_mine + gw_far.astype(F32)).astype(BF)
    cut = (gw.shape[0] + node_gw.shape[0]) // 2
    first, second = sum_over_patches(
        gw[:cut], jnp.concatenate([gw[cut:], node_gw], axis=0), torus
    )

    edge_grad, sum_mine, sum_theirs = call(
        edge_inputs, tiles,
        [rows_of(TILE, width), rows_of(TILE, width), cols_of(TILE), cols_of(TILE), whole((width, width))],
        [rows_of(TILE, width), whole((4 * rows, width)), whole((4 * rows, width))],
        [((edges, width), F32), ((4 * rows, width), F32), ((4 * rows, width), BF)],
        [((6 * rows, width), F32), ((2 * rows, width), F32)],
        "edge_inputs", 8 * sq, 6 << 20, 40,
    )(gpre, edge_cot, send_row, recv_row, edge_w1)

    sum_far = lax.ppermute(sum_theirs, "grp", other)
    both = (sum_mine[: 3 * rows] + sum_far[: 3 * rows].astype(F32)).astype(BF)
    from_next = lax.ppermute(both[:rows], "patch", down)
    from_prev = lax.ppermute(both[2 * rows :], "patch", up)
    node_grad = call(
        node_finish, 1,
        [whole((4 * rows, width)), whole((4 * rows, width)), whole((rows, width)),
         whole((rows, width)), whole((rows, width)), whole((3 * width, width))],
        [whole((rows, width))],
        [((rows, width), F32)],
        [],
        "node_finish", sq // 2, 2 << 20, 24,
    )(sum_mine, sum_far, from_next, from_prev, node_gin, edge_w1)[0]

    first, second = first.astype(F32), second.astype(F32)
    big, small, tail = 3 * width // 2, width // 2, 2 * width - cut
    return (
        node_grad,
        edge_grad,
        first[:big],
        jnp.concatenate([first[big:], second[:tail]], axis=0),
        second[tail : tail + width],
        second[tail + width :],
    )


def solution(mesh):
    split_rows = P(("patch", "grp"), None)
    flat = P(("patch", "grp"))
    in_specs = (split_rows,) * 4 + (P(),) * 6 + (flat,) * 3
    out_specs = (split_rows, split_rows) + (P("grp", None),) * 4
    return jax.shard_map(local, mesh=mesh, in_specs=in_specs, out_specs=out_specs, check_vma=False)
```

```python
import functools
import numpy as np
import jax
import jax.numpy as jnp
from jax import lax
from jax.experimental import pallas as pl
from jax.experimental.pallas import tpu as pltpu
from jax.sharding import PartitionSpec as P

EPS = 1e-05
F32 = jnp.float32
BF = jnp.bfloat16
TILE = 256


def mm(a, b):
    return jnp.dot(a, b, preferred_element_type=F32)


def mm_nt(a, b):
    return lax.dot_general(a, b, (((1,), (1,)), ((), ())), preferred_element_type=F32)


def mm_tn(a, b):
    return lax.dot_general(a, b, (((0,), (0,)), ((), ())), preferred_element_type=F32)


def split(x):
    high = x.astype(BF)
    return high, (x - high.astype(F32)).astype(BF)


def hot_rows(index, rows):
    grid = lax.broadcasted_iota(jnp.int32, (rows, index.shape[1]), 0)
    return jnp.where(grid == index, 1.0, 0.0).astype(BF)


def hot_cols(index, cols):
    grid = lax.broadcasted_iota(jnp.int32, (index.shape[0], cols), 1)
    return jnp.where(grid == index, 1.0, 0.0).astype(BF)


def sigmoid(x):
    return 1.0 / (1.0 + jnp.exp(-x))


def norm_forward(out):
    center = out - jnp.mean(out, axis=-1, keepdims=True)
    inv_std = lax.rsqrt(jnp.mean(center * center, axis=-1, keepdims=True) + EPS)
    return center * inv_std, inv_std


def norm_backward(grad_y, gain, normed, inv_std):
    scaled = grad_y * gain
    return inv_std * (
        scaled
        - jnp.mean(scaled, axis=-1, keepdims=True)
        - normed * jnp.mean(scaled * normed, axis=-1, keepdims=True)
    )


def alive(cnt_ref, step, tile):
    slot = step * tile + lax.broadcasted_iota(jnp.int32, (tile, 1), 0)
    return jnp.where(slot < cnt_ref[0], 1.0, 0.0)


def edge_forward(
    cnt_ref, lat_ref, near_ref, far_ref, sc_ref, rc_ref, rr_ref, w1_ref, w2_ref, gain_ref,
    ein_ref, pre_ref, out_ref, agg_ref, ext, own,
):
    step = pl.program_id(0)
    tile, width = lat_ref.shape
    half = near_ref.shape[0]
    rows = half // 3

    @pl.when(step == 0)
    def _():
        ext[:half] = near_ref[...]
        ext[half:] = far_ref[...]
        own[:rows] = near_ref[rows : 2 * rows]
        own[rows:] = far_ref[rows : 2 * rows]
        agg_ref[...] = jnp.zeros_like(agg_ref)

    ein_ref[:, :width] = lat_ref[...].astype(BF)
    ein_ref[:, width : 2 * width] = mm(hot_cols(sc_ref[...], 2 * half), ext[...]).astype(BF)
    ein_ref[:, 2 * width :] = mm(hot_cols(rc_ref[...], 2 * rows), own[...]).astype(BF)
    pre = mm(ein_ref[...], w1_ref[...])
    pre_ref[...] = pre
    out = mm((pre * sigmoid(pre)).astype(BF), w2_ref[...])
    out_ref[...] = out
    normed, _ = norm_forward(out)
    upd = normed * gain_ref[...] * alive(cnt_ref, step, tile)
    high, low = split(upd)
    hot = hot_rows(rr_ref[...], 2 * rows)
    agg_ref[...] += mm(hot, high) + mm(hot, low)


def node_both(
    g_ref, near_ref, far_ref, agg_ref, got_ref, cot_ref, cot_far_ref, w1_ref, w2_ref, gain_ref,
    gin_ref, gagg_ref, gw_ref, acts,
):
    rows = cot_ref.shape[0]
    width = cot_ref.shape[1]
    g = g_ref[0]
    nodes = jnp.concatenate([near_ref[rows : 2 * rows], far_ref[rows : 2 * rows]], axis=0)
    agg = jnp.concatenate(
        [agg_ref[:rows] + got_ref[rows:], agg_ref[rows:] + got_ref[:rows]], axis=0
    ).astype(BF)
    cot = jnp.concatenate([cot_ref[...], cot_far_ref[...]], axis=0)
    pre = mm(nodes, w1_ref[:width]) + mm(agg, w1_ref[width:])
    sig = sigmoid(pre)
    act = (pre * sig).astype(BF)
    acts[...] = act
    normed, inv_std = norm_forward(mm(act, w2_ref[...]))
    gout = norm_backward(cot, gain_ref[...], normed, inv_std).astype(BF)
    gpre = (mm_nt(gout, w2_ref[...]) * (sig * (1.0 + pre * (1.0 - sig)))).astype(BF)
    gin_ref[...] = cot_ref[...] + mm_nt(gpre[:rows], w1_ref[:width])
    gagg_ref[...] = mm_nt(gpre, w1_ref[width:])
    part = jnp.where(g == 0, nodes.astype(F32), agg.astype(F32)).astype(BF)
    gw_ref[:width] = mm_tn(part, gpre).astype(BF)
    some = acts[:, pl.ds(pl.multiple_of(g * (width // 2), 128), width // 2)]
    gw_ref[width:] = mm_tn(some, gout).astype(BF)


def edge_backward(
    cnt_ref, g_ref, cot_ref, gagg_ref, rc_ref, pre_ref, out_ref, ein_ref, w2_ref, gain_ref,
    gpre_ref, mine_ref, theirs_ref, high, low, acts, gouts, eins,
):
    step = pl.program_id(0)
    tile, width = cot_ref.shape

    @pl.when(step == 0)
    def _():
        a, b = split(gagg_ref[...])
        high[...] = a
        low[...] = b

    hot = hot_cols(rc_ref[...], gagg_ref.shape[0])
    grad = cot_ref[...] + (mm(hot, high[...]) + mm(hot, low[...]))
    grad = grad * alive(cnt_ref, step, tile)
    normed, inv_std = norm_forward(out_ref[...])
    gout = norm_backward(grad, gain_ref[...], normed, inv_std).astype(BF)
    pre = pre_ref[...]
    sig = sigmoid(pre)
    here = pl.ds(pl.multiple_of(step * tile, tile), tile)
    acts[here] = (pre * sig).astype(BF)
    gouts[here] = gout
    eins[here] = ein_ref[...]
    gpre_ref[here] = (mm_nt(gout, w2_ref[...]) * (sig * (1.0 + pre * (1.0 - sig)))).astype(BF)

    @pl.when(step == pl.num_programs(0) - 1)
    def _():
        big, small = 3 * width // 2, width // 2
        for k in range(2):
            side = g_ref[0] if k == 1 else 1 - g_ref[0]
            cols = eins[:, pl.ds(pl.multiple_of(side * big, 128), big)]
            some = acts[:, pl.ds(pl.multiple_of(side * small, 128), small)]
            first = mm_tn(cols, gpre_ref[...])
            second = mm_tn(some, gouts[...])
            dst = mine_ref if k == 1 else theirs_ref
            dst[:big] = first.astype(dst.dtype)
            dst[big:] = second.astype(dst.dtype)


def edge_inputs(
    gpre_ref, cot_ref, sr_ref, rr_ref, w1_ref, grad_ref, mine_ref, theirs_ref, sent, recvd,
):
    step = pl.program_id(0)
    width = cot_ref.shape[1]
    half, rows = sent.shape[0] // 2, recvd.shape[0] // 2

    @pl.when(step == 0)
    def _():
        sent[...] = jnp.zeros_like(sent)
        recvd[...] = jnp.zeros_like(recvd)

    gpre = gpre_ref[...]
    grad_ref[...] = cot_ref[...] + mm_nt(gpre, w1_ref[...])
    sent[...] += mm(hot_rows(sr_ref[...], 2 * half), gpre)
    recvd[...] += mm(hot_rows(rr_ref[...], 2 * rows), gpre)

    @pl.when(step == pl.num_programs(0) - 1)
    def _():
        mine_ref[:half] = sent[:half]
        mine_ref[half:] = recvd[:rows]
        theirs_ref[:half] = sent[half:].astype(BF)
        theirs_ref[half:] = recvd[rows:].astype(BF)


def whole(shape):
    return pl.BlockSpec(shape, lambda i: (0,) * len(shape))


def rows_of(tile, width):
    return pl.BlockSpec((tile, width), lambda i: (i, 0))


def cols_of(tile):
    return pl.BlockSpec((1, tile), lambda i: (0, i))


SMEM = pl.BlockSpec(memory_space=pltpu.SMEM)


def call(body, grid, ins, outs, shapes, scratch, name, flops, traffic, limit):
    return pl.pallas_call(
        body,
        grid=(grid,),
        in_specs=ins,
        out_specs=outs,
        out_shape=[jax.ShapeDtypeStruct(s, d) for s, d in shapes],
        scratch_shapes=[pltpu.VMEM(s, d) for s, d in scratch],
        name=name,
        cost_estimate=pl.CostEstimate(flops=flops, bytes_accessed=traffic, transcendentals=0),
        compiler_params=pltpu.CompilerParams(
            dimension_semantics=("arbitrary",), vmem_limit_bytes=limit << 20
        ),
    )


def node_finish(mine_ref, got_ref, next_ref, prev_ref, gin_ref, w1_ref, out_ref):
    rows, width = gin_ref.shape
    mid = slice(rows, 2 * rows)
    sent = mine_ref[mid] + got_ref[mid].astype(F32)
    sent = (sent + next_ref[...].astype(F32) + prev_ref[...].astype(F32)).astype(BF)
    recvd = (mine_ref[3 * rows :] + got_ref[3 * rows :].astype(F32)).astype(BF)
    out_ref[...] = (
        gin_ref[...]
        + mm_nt(sent, w1_ref[width : 2 * width])
        + mm_nt(recvd, w1_ref[2 * width :])
    )


def pack(slot_ref, mine_ref, far_ref, node_ref, own_ref, *sends):
    count = len(sends) + 1
    big, small = mine_ref.shape[0] * 3 // 4 // count, mine_ref.shape[0] // 4 // count
    wide, thin = node_ref.shape[0] * 2 // 3 // count, node_ref.shape[0] // 3 // count
    for j, dst in enumerate((own_ref,) + sends):
        at = slot_ref[j]
        rows = 0
        for size, base in ((big, 0), (small, big * count)):
            here = pl.ds(pl.multiple_of(base + at * size, 32), size)
            value = mine_ref[here] + far_ref[here].astype(F32)
            dst[rows : rows + size] = value.astype(BF)
            rows += size
        for size, base in ((wide, 0), (thin, wide * count)):
            here = pl.ds(pl.multiple_of(base + at * size, 32), size)
            dst[rows : rows + size] = node_ref[here]
            rows += size


def unpack(slot_ref, *refs):
    parts, (first_ref, second_ref, third_ref, fourth_ref) = refs[:-4], refs[-4:]
    count = len(parts)
    for j, part in enumerate(parts):
        rows = 0
        for dst in (first_ref, second_ref, third_ref, fourth_ref):
            size = dst.shape[0] // count
            here = pl.ds(pl.multiple_of(slot_ref[j] * size, 32), size)
            dst[here] = part[rows : rows + size].astype(F32)
            rows += size


def sum_and_split(count, slot_ref, own_ref, *refs):
    got, total, sends = refs[:count], refs[-1], refs[count:-1]
    value = own_ref[...].astype(F32)
    for part in got:
        value = value + part[...].astype(F32)
    total[...] = value
    size = sends[0].shape[0]
    for j, dst in enumerate(sends):
        here = pl.ds(pl.multiple_of(slot_ref[j] * size, 8), size)
        dst[...] = total[here].astype(dst.dtype)


def join(slot_ref, *refs):
    parts, dst = refs[:-1], refs[-1]
    size = parts[0].shape[0]
    for j, part in enumerate(parts):
        here = pl.ds(pl.multiple_of(slot_ref[j] * size, 8), size)
        dst[here] = part[...].astype(dst.dtype)


def small_call(body, args, shapes, scratch, name):
    return call(
        body, 1, [SMEM] + [whole(a.shape) for a in args[1:]], [whole(s) for s, _ in shapes],
        shapes, scratch, name, 1 << 20, sum(int(np.prod(s)) * 4 for s, _ in shapes), 24,
    )(*args)


def sum_over_patches(mine, far, node, sizes):
    nz, ny, nx = sizes
    width = mine.shape[1]
    where, g = lax.axis_index("patch"), lax.axis_index("grp")
    x, y, z = lax.rem(where, nx), lax.rem(lax.div(where, nx), ny), lax.div(where, nx * ny)
    n = nx
    at = (jnp.where(g == 0, x, y), jnp.where(g == 0, y, x))
    steps = [s for k in range(1, n // 2 + 1) for s in (k, -k)][: n - 1]

    def send(value, move):
        pairs = []
        for source in range(2 * nz * ny * nx):
            to = move(*[int(v) for v in np.unravel_index(source, (nz, ny, nx, 2))])
            pairs.append((source, int(np.ravel_multi_index(to, (nz, ny, nx, 2)))))
        return lax.ppermute(value, ("patch", "grp"), pairs)

    def shift(value, leg, s):
        def move(z, y, x, g):
            return (z, y, (x + s) % nx, g) if g == leg else (z, (y + s) % ny, x, g)

        return send(value, move)

    def slots(leg, sign):
        return jnp.stack([at[leg]] + [lax.rem(at[leg] + sign * s + n, n) for s in steps]).astype(jnp.int32)

    def flip(value, partner):
        return send(value, lambda z, y, x, g: (partner[z], y, x, g))

    rows = (mine.shape[0] + node.shape[0]) // n
    own, *out = small_call(
        pack, (slots(0, 1), mine, far, node), [((rows, width), BF)] * n, [], "pack"
    )
    got = [shift(v, 0, s) for v, s in zip(out, steps)]
    own, *out = small_call(
        functools.partial(sum_and_split, n - 1), (slots(1, 1), own, *got),
        [((rows // n, width), F32)] + [((rows // n, width), BF)] * (n - 1),
        [((rows, width), F32)], "sum_first",
    )
    got = [shift(v, 1, s) for v, s in zip(out, steps)]
    rows //= n
    near = [k ^ 1 for k in range(nz)]
    next_to = [(k + 1) % nz if k % 2 else (k - 1) % nz for k in range(nz)]
    across = [(k // 4) * 4 + 3 - k % 4 if k % 4 in (0, 3) else nz - 1 - k for k in range(nz)]
    bit = jnp.bitwise_and(jnp.bitwise_xor(lax.div(z, 2), z), 1)
    halves = jnp.stack([bit, 1 - bit]).astype(jnp.int32)
    keep, out = small_call(
        functools.partial(sum_and_split, n - 1), (halves, own, *got),
        [((rows // 2, width), F32), ((rows // 2, width), BF)],
        [((rows, width), F32)], "sum_second",
    )
    part = (keep + flip(out, near).astype(F32)).astype(BF)
    part = (part.astype(F32) + flip(part, next_to).astype(F32)).astype(BF)
    part = (part.astype(F32) + flip(part, across).astype(F32)).astype(BF)
    (part,) = small_call(
        join, (halves, part, flip(part, near)), [((rows, width), BF)], [], "join_z"
    )
    (part,) = small_call(
        join, (slots(1, -1), part, *[shift(part, 1, s) for s in steps]),
        [((rows * n, width), BF)], [], "join_second",
    )
    tall, short = mine.shape[0] // 4, node.shape[0] // 3
    return small_call(
        unpack, (slots(0, -1), part, *[shift(part, 0, s) for s in steps]),
        [((3 * tall, width), F32), ((tall, width), F32), ((2 * short, width), F32), ((short, width), F32)],
        [], "unpack",
    )


def local(
    node_latent, edge_latent, node_cot, edge_cot, edge_w1, edge_w2, edge_gain,
    node_w1, node_w2, node_gain, senders, receivers, counts,
):
    rows, width = node_latent.shape
    edges = edge_latent.shape[0]
    tiles = edges // TILE
    n_patch = lax.axis_size("patch")
    g = lax.axis_index("grp").astype(jnp.int32)
    other = [(0, 1), (1, 0)]
    up = [(i, (i + 1) % n_patch) for i in range(n_patch)]
    down = [(j, i) for i, j in up]

    node_bf = node_latent.astype(BF)
    before = lax.ppermute(node_bf, "patch", up)
    after = lax.ppermute(node_bf, "patch", down)
    near = jnp.concatenate([before, node_bf, after], axis=0)
    far = lax.ppermute(near, "grp", other)
    cot_far = lax.ppermute(node_cot, "grp", other)

    slab, place = senders // (2 * rows), senders % (2 * rows)
    side = jnp.where(place // rows == g, 0, 3 * rows)
    send_at = side + slab * rows + place % rows
    recv_at = jnp.where(receivers // rows == g, 0, rows) + receivers % rows
    send_col, send_row = send_at[:, None], send_at[None, :]
    recv_col, recv_row = recv_at[:, None], recv_at[None, :]
    egain, ngain = edge_gain[None, :], node_gain[None, :]
    which = g[None]

    sq = edges * width * width
    edge_in, edge_pre, edge_out, agg = call(
        edge_forward, tiles,
        [SMEM, rows_of(TILE, width), whole((3 * rows, width)), whole((3 * rows, width)),
         rows_of(TILE, 1), rows_of(TILE, 1), cols_of(TILE),
         whole((3 * width, width)), whole((width, width)), whole((1, width))],
        [rows_of(TILE, 3 * width), rows_of(TILE, width), rows_of(TILE, width), whole((2 * rows, width))],
        [((edges, 3 * width), BF), ((edges, width), F32), ((edges, width), F32), ((2 * rows, width), F32)],
        [((6 * rows, width), BF), ((2 * rows, width), BF)],
        "edge_forward", 14 * sq, 12 << 20, 60,
    )(counts, edge_latent, near, far, send_col, recv_col, recv_row, edge_w1, edge_w2, egain)

    agg_far = lax.ppermute(agg, "grp", other)
    node_gin, gagg, node_gw = call(
        node_both, 1,
        [SMEM, whole((3 * rows, width)), whole((3 * rows, width)), whole((2 * rows, width)),
         whole((2 * rows, width)), whole((rows, width)), whole((rows, width)),
         whole((2 * width, width)), whole((width, width)), whole((1, width))],
        [whole((rows, width)), whole((2 * rows, width)), whole((3 * width // 2, width))],
        [((rows, width), F32), ((2 * rows, width), F32), ((3 * width // 2, width), BF)],
        [((2 * rows, width), BF)],
        "node_both", 5 * sq, 6 << 20, 40,
    )(which, near, far, agg, agg_far, node_cot, cot_far, node_w1, node_w2, ngain)

    gpre, gw_mine, gw_theirs = call(
        edge_backward, tiles,
        [SMEM, SMEM, rows_of(TILE, width), whole((2 * rows, width)), rows_of(TILE, 1),
         rows_of(TILE, width), rows_of(TILE, width), rows_of(TILE, 3 * width),
         whole((width, width)), whole((1, width))],
        [whole((edges, width)), whole((2 * width, width)), whole((2 * width, width))],
        [((edges, width), BF), ((2 * width, width), F32), ((2 * width, width), BF)],
        [((2 * rows, width), BF), ((2 * rows, width), BF), ((edges, width), BF), ((edges, width), BF),
         ((edges, 3 * width), BF)],
        "edge_backward", 12 * sq, 14 << 20, 60,
    )(counts, which, edge_cot, gagg, recv_col, edge_pre, edge_out, edge_in, edge_w2, egain)

    gw_far = lax.ppermute(gw_theirs, "grp", other)
    weights = sum_over_patches(gw_mine, gw_far, node_gw, (n_patch // 16, 4, 4))

    edge_grad, sum_mine, sum_theirs = call(
        edge_inputs, tiles,
        [rows_of(TILE, width), rows_of(TILE, width), cols_of(TILE), cols_of(TILE), whole((width, width))],
        [rows_of(TILE, width), whole((4 * rows, width)), whole((4 * rows, width))],
        [((edges, width), F32), ((4 * rows, width), F32), ((4 * rows, width), BF)],
        [((6 * rows, width), F32), ((2 * rows, width), F32)],
        "edge_inputs", 8 * sq, 6 << 20, 60,
    )(gpre, edge_cot, send_row, recv_row, edge_w1)

    sum_far = lax.ppermute(sum_theirs, "grp", other)
    both = (sum_mine[: 3 * rows] + sum_far[: 3 * rows].astype(F32)).astype(BF)
    from_next = lax.ppermute(both[:rows], "patch", down)
    from_prev = lax.ppermute(both[2 * rows :], "patch", up)
    node_grad = call(
        node_finish, 1,
        [whole((4 * rows, width)), whole((4 * rows, width)), whole((rows, width)),
         whole((rows, width)), whole((rows, width)), whole((3 * width, width))],
        [whole((rows, width))],
        [((rows, width), F32)],
        [],
        "node_finish", sq // 2, 2 << 20, 24,
    )(sum_mine, sum_far, from_next, from_prev, node_gin, edge_w1)[0]

    return (node_grad, edge_grad, *weights)


def solution(mesh):
    split_rows = P(("patch", "grp"), None)
    flat = P(("patch", "grp"))
    in_specs = (split_rows,) * 4 + (P(),) * 6 + (flat,) * 3
    out_specs = (split_rows, split_rows) + (P("grp", None),) * 4
    return jax.shard_map(local, mesh=mesh, in_specs=in_specs, out_specs=out_specs, check_vma=False)
```

```python
import functools
import numpy as np
import jax
import jax.numpy as jnp
from jax import lax
from jax.experimental import pallas as pl
from jax.experimental.pallas import tpu as pltpu
from jax.sharding import PartitionSpec as P


EPS = 1e-05
F32 = jnp.float32
BF = jnp.bfloat16
TILE = 256


def mm(a, b):
    return jnp.dot(a, b, preferred_element_type=F32)


def mm_nt(a, b):
    return lax.dot_general(a, b, (((1,), (1,)), ((), ())), preferred_element_type=F32)


def mm_tn(a, b):
    return lax.dot_general(a, b, (((0,), (0,)), ((), ())), preferred_element_type=F32)


def split(x):
    high = x.astype(BF)
    return high, (x - high.astype(F32)).astype(BF)


def hot_rows(index, rows):
    grid = lax.broadcasted_iota(jnp.int32, (rows, index.shape[1]), 0)
    return jnp.where(grid == index, 1.0, 0.0).astype(BF)


def hot_cols(index, cols):
    grid = lax.broadcasted_iota(jnp.int32, (index.shape[0], cols), 1)
    return jnp.where(grid == index, 1.0, 0.0).astype(BF)


def sigmoid(x):
    return 1.0 / (1.0 + jnp.exp(-x))


def norm_forward(out):
    center = out - jnp.mean(out, axis=-1, keepdims=True)
    inv_std = lax.rsqrt(jnp.mean(center * center, axis=-1, keepdims=True) + EPS)
    return center * inv_std, inv_std


def norm_backward(grad_y, gain, normed, inv_std):
    scaled = grad_y * gain
    return inv_std * (
        scaled
        - jnp.mean(scaled, axis=-1, keepdims=True)
        - normed * jnp.mean(scaled * normed, axis=-1, keepdims=True)
    )


def alive(cnt_ref, step, tile):
    slot = step * tile + lax.broadcasted_iota(jnp.int32, (tile, 1), 0)
    return jnp.where(slot < cnt_ref[0], 1.0, 0.0)


def edge_forward(
    cnt_ref, lat_ref, near_ref, far_ref, sc_ref, rc_ref, rr_ref, w1_ref, w2_ref, gain_ref,
    ein_ref, pre_ref, out_ref, agg_ref, ext, own,
):
    step = pl.program_id(0)
    tile, width = lat_ref.shape
    half = near_ref.shape[0]
    rows = half // 3

    @pl.when(step == 0)
    def _():
        ext[:half] = near_ref[...]
        ext[half:] = far_ref[...]
        own[:rows] = near_ref[rows : 2 * rows]
        own[rows:] = far_ref[rows : 2 * rows]
        agg_ref[...] = jnp.zeros_like(agg_ref)

    ein_ref[:, :width] = lat_ref[...].astype(BF)
    ein_ref[:, width : 2 * width] = mm(hot_cols(sc_ref[...], 2 * half), ext[...]).astype(BF)
    ein_ref[:, 2 * width :] = mm(hot_cols(rc_ref[...], 2 * rows), own[...]).astype(BF)
    pre = mm(ein_ref[...], w1_ref[...])
    pre_ref[...] = pre
    out = mm((pre * sigmoid(pre)).astype(BF), w2_ref[...])
    out_ref[...] = out
    normed, _ = norm_forward(out)
    upd = normed * gain_ref[...] * alive(cnt_ref, step, tile)
    high, low = split(upd)
    hot = hot_rows(rr_ref[...], 2 * rows)
    agg_ref[...] += mm(hot, high) + mm(hot, low)


def node_both(
    g_ref, near_ref, far_ref, agg_ref, got_ref, cot_ref, cot_far_ref, w1_ref, w2_ref, gain_ref,
    gin_ref, gagg_ref, gw_ref, acts,
):
    rows = cot_ref.shape[0]
    width = cot_ref.shape[1]
    g = g_ref[0]
    nodes = jnp.concatenate([near_ref[rows : 2 * rows], far_ref[rows : 2 * rows]], axis=0)
    agg = jnp.concatenate(
        [agg_ref[:rows] + got_ref[rows:], agg_ref[rows:] + got_ref[:rows]], axis=0
    ).astype(BF)
    cot = jnp.concatenate([cot_ref[...], cot_far_ref[...]], axis=0)
    pre = mm(nodes, w1_ref[:width]) + mm(agg, w1_ref[width:])
    sig = sigmoid(pre)
    act = (pre * sig).astype(BF)
    acts[...] = act
    normed, inv_std = norm_forward(mm(act, w2_ref[...]))
    gout = norm_backward(cot, gain_ref[...], normed, inv_std).astype(BF)
    gpre = (mm_nt(gout, w2_ref[...]) * (sig * (1.0 + pre * (1.0 - sig)))).astype(BF)
    gin_ref[...] = cot_ref[...] + mm_nt(gpre[:rows], w1_ref[:width])
    gagg_ref[...] = mm_nt(gpre, w1_ref[width:])
    part = jnp.where(g == 0, nodes.astype(F32), agg.astype(F32)).astype(BF)
    gw_ref[:width] = mm_tn(part, gpre).astype(BF)
    some = acts[:, pl.ds(pl.multiple_of(g * (width // 2), 128), width // 2)]
    gw_ref[width:] = mm_tn(some, gout).astype(BF)


def edge_backward(
    cnt_ref, g_ref, cot_ref, gagg_ref, rc_ref, pre_ref, out_ref, ein_ref, w2_ref, gain_ref, node_ref,
    gpre_ref, mine_ref, theirs_ref, high, low, acts, gouts, eins,
):
    step = pl.program_id(0)
    tile, width = cot_ref.shape

    @pl.when(step == 0)
    def _():
        a, b = split(gagg_ref[...])
        high[...] = a
        low[...] = b

    hot = hot_cols(rc_ref[...], gagg_ref.shape[0])
    grad = cot_ref[...] + (mm(hot, high[...]) + mm(hot, low[...]))
    grad = grad * alive(cnt_ref, step, tile)
    normed, inv_std = norm_forward(out_ref[...])
    gout = norm_backward(grad, gain_ref[...], normed, inv_std).astype(BF)
    pre = pre_ref[...]
    sig = sigmoid(pre)
    here = pl.ds(pl.multiple_of(step * tile, tile), tile)
    acts[here] = (pre * sig).astype(BF)
    gouts[here] = gout
    eins[here] = ein_ref[...]
    gpre_ref[here] = (mm_nt(gout, w2_ref[...]) * (sig * (1.0 + pre * (1.0 - sig)))).astype(BF)

    @pl.when(step == pl.num_programs(0) - 1)
    def _():
        big, small = 3 * width // 2, width // 2
        mine_ref[2 * width :] = node_ref[...]
        for k in range(2):
            side = g_ref[0] if k == 1 else 1 - g_ref[0]
            cols = eins[:, pl.ds(pl.multiple_of(side * big, 128), big)]
            some = acts[:, pl.ds(pl.multiple_of(side * small, 128), small)]
            first = mm_tn(cols, gpre_ref[...])
            second = mm_tn(some, gouts[...])
            dst = mine_ref if k == 1 else theirs_ref
            dst[:big] = first.astype(dst.dtype)
            dst[big : big + small] = second.astype(dst.dtype)


def edge_inputs(
    gpre_ref, cot_ref, sr_ref, rr_ref, w1_ref, grad_ref, mine_ref, theirs_ref, sent, recvd,
):
    step = pl.program_id(0)
    half, rows = sent.shape[0] // 2, recvd.shape[0] // 2

    @pl.when(step == 0)
    def _():
        sent[...] = jnp.zeros_like(sent)
        recvd[...] = jnp.zeros_like(recvd)

    gpre = gpre_ref[...]
    grad_ref[...] = cot_ref[...] + mm_nt(gpre, w1_ref[...])
    sent[...] += mm(hot_rows(sr_ref[...], 2 * half), gpre)
    recvd[...] += mm(hot_rows(rr_ref[...], 2 * rows), gpre)

    @pl.when(step == pl.num_programs(0) - 1)
    def _():
        mine_ref[:half] = sent[:half]
        mine_ref[half:] = recvd[:rows]
        theirs_ref[:half] = sent[half:].astype(BF)
        theirs_ref[half:] = recvd[rows:].astype(BF)


def whole(shape):
    return pl.BlockSpec(shape, lambda i: (0,) * len(shape))


def rows_of(tile, width):
    return pl.BlockSpec((tile, width), lambda i: (i, 0))


def cols_of(tile):
    return pl.BlockSpec((1, tile), lambda i: (0, i))


SMEM = pl.BlockSpec(memory_space=pltpu.SMEM)


def call(body, grid, ins, outs, shapes, scratch, flops, traffic, limit):
    return pl.pallas_call(
        body,
        grid=(grid,),
        in_specs=ins,
        out_specs=outs,
        out_shape=[jax.ShapeDtypeStruct(s, d) for s, d in shapes],
        scratch_shapes=[pltpu.VMEM(s, d) for s, d in scratch],
        cost_estimate=pl.CostEstimate(flops=flops, bytes_accessed=traffic, transcendentals=0),
        compiler_params=pltpu.CompilerParams(
            dimension_semantics=("arbitrary",), vmem_limit_bytes=limit << 20
        ),
    )


def node_finish(mine_ref, got_ref, next_ref, prev_ref, gin_ref, ws_ref, wr_ref, out_ref):
    rows = gin_ref.shape[0]
    mid = slice(rows, 2 * rows)
    sent = mine_ref[mid] + got_ref[mid].astype(F32)
    sent = (sent + next_ref[...].astype(F32) + prev_ref[...].astype(F32)).astype(BF)
    recvd = (mine_ref[3 * rows :] + got_ref[3 * rows :].astype(F32)).astype(BF)
    out_ref[...] = (
        gin_ref[...]
        + mm_nt(sent, ws_ref[...])
        + mm_nt(recvd, wr_ref[...])
    )


def pack(slot_ref, mine_ref, far_ref, own_ref, *sends):
    count = len(sends) + 1
    edge = far_ref.shape[0]
    node = mine_ref.shape[0] - edge
    for j, dst in enumerate((own_ref,) + sends):
        rows, base = 0, 0
        for whole_size in (3 * edge // 4, edge // 4, 2 * node // 3, node // 3):
            size = whole_size // count
            here = pl.ds(pl.multiple_of(base + slot_ref[j] * size, 32), size)
            value = mine_ref[here]
            if base < edge:
                value = (value.astype(F32) + far_ref[here].astype(F32)).astype(BF)
            dst[rows : rows + size] = value
            rows += size
            base += whole_size


def unpack(slot_ref, *refs):
    parts, (first_ref, second_ref, third_ref, fourth_ref) = refs[:-4], refs[-4:]
    count = len(parts)
    for j, part in enumerate(parts):
        rows = 0
        for dst in (first_ref, second_ref, third_ref, fourth_ref):
            size = dst.shape[0] // count
            here = pl.ds(pl.multiple_of(slot_ref[j] * size, 32), size)
            dst[here] = part[rows : rows + size].astype(F32)
            rows += size


def sum_and_split(count, slot_ref, own_ref, *refs):
    got, total, sends = refs[:count], refs[-1], refs[count:-1]
    value = own_ref[...].astype(F32)
    for part in got:
        value = value + part[...].astype(F32)
    total[...] = value
    size = sends[0].shape[0]
    for j, dst in enumerate(sends):
        here = pl.ds(pl.multiple_of(slot_ref[j] * size, 8), size)
        dst[...] = total[here].astype(dst.dtype)


def join(slot_ref, *refs):
    parts, dst = refs[:-1], refs[-1]
    size = parts[0].shape[0]
    for j, part in enumerate(parts):
        here = pl.ds(pl.multiple_of(slot_ref[j] * size, 8), size)
        dst[here] = part[...].astype(dst.dtype)


def small_call(body, args, shapes, scratch):
    return call(
        body, 1, [SMEM] + [whole(a.shape) for a in args[1:]], [whole(s) for s, _ in shapes],
        shapes, scratch, 1 << 20, sum(int(np.prod(s)) * 4 for s, _ in shapes), 12,
    )(*args)


def sum_over_patches(mine, far, sizes, others):
    nz, ny, nx = sizes
    width = mine.shape[1]
    where, g = lax.axis_index("patch"), lax.axis_index("grp")
    x, y, z = lax.rem(where, nx), lax.rem(lax.div(where, nx), ny), lax.div(where, nx * ny)
    n = nx
    at = (jnp.where(g == 0, x, y), jnp.where(g == 0, y, x))
    steps = [s for k in range(1, n // 2 + 1) for s in (k, -k)][: n - 1]

    def send(value, move):
        pairs = []
        for source in range(2 * nz * ny * nx):
            to = move(*[int(v) for v in np.unravel_index(source, (nz, ny, nx, 2))])
            pairs.append((source, int(np.ravel_multi_index(to, (nz, ny, nx, 2)))))
        return lax.ppermute(value, ("patch", "grp"), pairs)

    def shift(value, leg, s):
        def move(z, y, x, g):
            return (z, y, (x + s) % nx, g) if g == leg else (z, (y + s) % ny, x, g)

        return send(value, move)

    def slots(leg, sign):
        return jnp.stack([at[leg]] + [lax.rem(at[leg] + sign * s + n, n) for s in steps]).astype(jnp.int32)

    def flip(value, partner):
        return send(value, lambda z, y, x, g: (partner[z], y, x, g))

    rows = mine.shape[0] // n
    own, *out = small_call(pack, (slots(0, 1), mine, far), [((rows, width), BF)] * n, [])
    got = [shift(v, 0, s) for v, s in zip(out, steps)]
    inputs = others.inputs()
    own, *out = small_call(
        functools.partial(sum_and_split, n - 1), (slots(1, 1), own, *got),
        [((rows // n, width), F32)] + [((rows // n, width), BF)] * (n - 1),
        [((rows, width), F32)],
    )
    got = [shift(v, 1, s) for v, s in zip(out, steps)]
    sums = others.swap(inputs)
    rows //= n
    near = [k ^ 1 for k in range(nz)]
    next_to = [(k + 1) % nz if k % 2 else (k - 1) % nz for k in range(nz)]
    across = [(k // 4) * 4 + 3 - k % 4 if k % 4 in (0, 3) else nz - 1 - k for k in range(nz)]
    bit = jnp.bitwise_and(jnp.bitwise_xor(lax.div(z, 2), z), 1)
    halves = jnp.stack([bit, 1 - bit]).astype(jnp.int32)
    keep, out = small_call(
        functools.partial(sum_and_split, n - 1), (halves, own, *got),
        [((rows // 2, width), F32), ((rows // 2, width), BF)],
        [((rows, width), F32)],
    )
    part = (keep + flip(out, near).astype(F32)).astype(BF)
    sums = others.shift(sums)
    part = (part.astype(F32) + flip(part, next_to).astype(F32)).astype(BF)
    part = (part.astype(F32) + flip(part, across).astype(F32)).astype(BF)
    node_grad = others.finish(sums)
    (part,) = small_call(join, (halves, part, flip(part, near)), [((rows, width), BF)], [])
    (part,) = small_call(
        join, (slots(1, -1), part, *[shift(part, 1, s) for s in steps]),
        [((rows * n, width), BF)], [],
    )
    tall = far.shape[0] // 4
    short = (mine.shape[0] - far.shape[0]) // 3
    weights = small_call(
        unpack, (slots(0, -1), part, *[shift(part, 0, s) for s in steps]),
        [((3 * tall, width), F32), ((tall, width), F32), ((2 * short, width), F32), ((short, width), F32)],
        [],
    )
    return node_grad, inputs[0], *weights


class Others:
    def __init__(self, inputs, swap, shift, finish):
        self.inputs, self.swap, self.shift, self.finish = inputs, swap, shift, finish


def local(
    node_latent, edge_latent, node_cot, edge_cot, edge_w1, edge_w2, edge_gain,
    node_w1, node_w2, node_gain, senders, receivers, counts,
):
    rows, width = node_latent.shape
    edges = edge_latent.shape[0]
    tiles = edges // TILE
    n_patch = lax.axis_size("patch")
    g = lax.axis_index("grp").astype(jnp.int32)
    other = [(0, 1), (1, 0)]
    up = [(i, (i + 1) % n_patch) for i in range(n_patch)]
    down = [(j, i) for i, j in up]

    node_bf = node_latent.astype(BF)
    before = lax.ppermute(node_bf, "patch", up)
    after = lax.ppermute(node_bf, "patch", down)
    near = jnp.concatenate([before, node_bf, after], axis=0)
    far = lax.ppermute(near, "grp", other)
    cot_far = lax.ppermute(node_cot, "grp", other)

    slab, place = senders // (2 * rows), senders % (2 * rows)
    side = jnp.where(place // rows == g, 0, 3 * rows)
    send_at = side + slab * rows + place % rows
    recv_at = jnp.where(receivers // rows == g, 0, rows) + receivers % rows
    send_col, send_row = send_at[:, None], send_at[None, :]
    recv_col, recv_row = recv_at[:, None], recv_at[None, :]
    egain, ngain = edge_gain[None, :], node_gain[None, :]
    which = g[None]

    sq = edges * width * width
    edge_in, edge_pre, edge_out, agg = call(
        edge_forward, tiles,
        [SMEM, rows_of(TILE, width), whole((3 * rows, width)), whole((3 * rows, width)),
         rows_of(TILE, 1), rows_of(TILE, 1), cols_of(TILE),
         whole((3 * width, width)), whole((width, width)), whole((1, width))],
        [rows_of(TILE, 3 * width), rows_of(TILE, width), rows_of(TILE, width), whole((2 * rows, width))],
        [((edges, 3 * width), BF), ((edges, width), F32), ((edges, width), F32), ((2 * rows, width), F32)],
        [((6 * rows, width), BF), ((2 * rows, width), BF)],
        14 * sq, 12 << 20, 20,
    )(counts, edge_latent, near, far, send_col, recv_col, recv_row, edge_w1, edge_w2, egain)

    agg_far = lax.ppermute(agg, "grp", other)
    node_gin, gagg, node_gw = call(
        node_both, 1,
        [SMEM, whole((3 * rows, width)), whole((3 * rows, width)), whole((2 * rows, width)),
         whole((2 * rows, width)), whole((rows, width)), whole((rows, width)),
         whole((2 * width, width)), whole((width, width)), whole((1, width))],
        [whole((rows, width)), whole((2 * rows, width)), whole((3 * width // 2, width))],
        [((rows, width), F32), ((2 * rows, width), F32), ((3 * width // 2, width), BF)],
        [((2 * rows, width), BF)],
        5 * sq, 6 << 20, 20,
    )(which, near, far, agg, agg_far, node_cot, cot_far, node_w1, node_w2, ngain)

    gpre, gw_mine, gw_theirs = call(
        edge_backward, tiles,
        [SMEM, SMEM, rows_of(TILE, width), whole((2 * rows, width)), rows_of(TILE, 1),
         rows_of(TILE, width), rows_of(TILE, width), rows_of(TILE, 3 * width),
         whole((width, width)), whole((1, width)),
         whole((3 * width // 2, width))],
        [whole((edges, width)), whole((7 * width // 2, width)), whole((2 * width, width))],
        [((edges, width), BF), ((7 * width // 2, width), BF), ((2 * width, width), BF)],
        [((2 * rows, width), BF), ((2 * rows, width), BF), ((edges, width), BF), ((edges, width), BF),
         ((edges, 3 * width), BF)],
        12 * sq, 14 << 20, 20,
    )(counts, which, edge_cot, gagg, recv_col, edge_pre, edge_out, edge_in, edge_w2, egain, node_gw)

    gw_far = lax.ppermute(gw_theirs, "grp", other)

    def inputs():
        return call(
            edge_inputs, tiles,
            [rows_of(TILE, width), rows_of(TILE, width), cols_of(TILE), cols_of(TILE), whole((width, width))],
            [rows_of(TILE, width), whole((4 * rows, width)), whole((4 * rows, width))],
            [((edges, width), F32), ((4 * rows, width), F32), ((4 * rows, width), BF)],
            [((6 * rows, width), F32), ((2 * rows, width), F32)],
            8 * sq, 6 << 20, 16,
        )(gpre, edge_cot, send_row, recv_row, edge_w1)

    def swap(made):
        return made[1], lax.ppermute(made[2], "grp", other)

    def shift(sums):
        mine, far = sums
        ends = [
            (mine[at : at + rows] + far[at : at + rows].astype(F32)).astype(BF) for at in (0, 2 * rows)
        ]
        return (
            mine, far,
            lax.ppermute(ends[0], "patch", down),
            lax.ppermute(ends[1], "patch", up),
        )

    def finish(sums):
        return call(
            node_finish, 1,
            [whole((4 * rows, width)), whole((4 * rows, width)), whole((rows, width)),
             whole((rows, width)), whole((rows, width)),
             pl.BlockSpec((width, width), lambda i: (1, 0)), pl.BlockSpec((width, width), lambda i: (2, 0))],
            [whole((rows, width))],
            [((rows, width), F32)],
            [],
            sq // 2, 2 << 20, 16,
        )(*sums, node_gin, edge_w1, edge_w1)[0]

    return sum_over_patches(
        gw_mine, gw_far, (n_patch // 16, 4, 4), Others(inputs, swap, shift, finish)
    )


def solution(mesh):
    split_rows = P(("patch", "grp"), None)
    flat = P(("patch", "grp"))
    in_specs = (split_rows,) * 4 + (P(),) * 6 + (flat,) * 3
    out_specs = (split_rows, split_rows) + (P("grp", None),) * 4

    return jax.shard_map(local, mesh=mesh, in_specs=in_specs, out_specs=out_specs, check_vma=False)
```

```python
import functools
import numpy as np
import jax
import jax.numpy as jnp
from jax import lax
from jax.experimental import pallas as pl
from jax.experimental.pallas import tpu as pltpu
from jax.sharding import PartitionSpec as P


EPS = 1e-05
F32 = jnp.float32
BF = jnp.bfloat16
TILE = 256
CORE = 18


def mm(a, b):
    return jnp.dot(a, b, preferred_element_type=F32)


def mm_nt(a, b):
    return lax.dot_general(a, b, (((1,), (1,)), ((), ())), preferred_element_type=F32)


def mm_tn(a, b):
    return lax.dot_general(a, b, (((0,), (0,)), ((), ())), preferred_element_type=F32)


def split(x):
    high = x.astype(BF)
    return high, (x - high.astype(F32)).astype(BF)


def hot_rows(index, rows):
    grid = lax.broadcasted_iota(jnp.int32, (rows, index.shape[1]), 0)
    return jnp.where(grid == index, 1.0, 0.0).astype(BF)


def hot_cols(index, cols):
    grid = lax.broadcasted_iota(jnp.int32, (index.shape[0], cols), 1)
    return jnp.where(grid == index, 1.0, 0.0).astype(BF)


def sigmoid(x):
    return 1.0 / (1.0 + jnp.exp(-x))


def norm_forward(out):
    center = out - jnp.mean(out, axis=-1, keepdims=True)
    inv_std = lax.rsqrt(jnp.mean(center * center, axis=-1, keepdims=True) + EPS)
    return center * inv_std, inv_std


def norm_backward(grad_y, gain, normed, inv_std):
    scaled = grad_y * gain
    return inv_std * (
        scaled
        - jnp.mean(scaled, axis=-1, keepdims=True)
        - normed * jnp.mean(scaled * normed, axis=-1, keepdims=True)
    )


def sender_place(index, core, rows):
    slab = jnp.where(index >= 2 * rows, 1, 0) + jnp.where(index >= 4 * rows, 1, 0)
    index = index - slab * (2 * rows)
    side = jnp.where(index >= rows, 1, 0)
    return jnp.where(side == core, 0, 3 * rows) + slab * rows + index - side * rows


def receiver_place(index, core, rows):
    side = jnp.where(index >= rows, 1, 0)
    return jnp.where(side == core, 0, rows) + index - side * rows


def alive(cnt_ref, step, tile):
    slot = step * tile + lax.broadcasted_iota(jnp.int32, (tile, 1), 0)
    return jnp.where(slot < cnt_ref[0], 1.0, 0.0)


def edge_first(table_ref, lat_ref, w1_ref, low_ref, part_ref):
    low = lat_ref[...].astype(BF)
    low_ref[...] = low
    part_ref[...] = mm(low, w1_ref[...])


def edge_forward(
    cnt_ref, g_ref, part_ref, a_ref, b_ref, c_ref, d_ref, e_ref, f_ref, sc_ref, rc_ref, rr_ref,
    ws_ref, wr_ref, w2_ref, gain_ref,
    ein_ref, pre_ref, out_ref, agg_ref, ext, own,
):
    step = pl.program_id(0)
    tile, width = part_ref.shape
    rows = a_ref.shape[0]

    @pl.when(step == 0)
    def _():
        for j, ref in enumerate((a_ref, b_ref, c_ref, d_ref, e_ref, f_ref)):
            ext[j * rows : (j + 1) * rows] = ref[...]
        own[:rows] = b_ref[...]
        own[rows:] = e_ref[...]
        agg_ref[...] = jnp.zeros_like(agg_ref)

    core = g_ref[CORE]
    sent = mm(hot_cols(sender_place(sc_ref[...], core, rows), 6 * rows), ext[...]).astype(BF)
    recvd = mm(hot_cols(receiver_place(rc_ref[...], core, rows), 2 * rows), own[...]).astype(BF)
    ein_ref[:, :width] = sent
    ein_ref[:, width:] = recvd
    pre = part_ref[...] + mm(sent, ws_ref[...]) + mm(recvd, wr_ref[...])
    pre_ref[...] = pre
    out = mm((pre * sigmoid(pre)).astype(BF), w2_ref[...])
    out_ref[...] = out
    normed, _ = norm_forward(out)
    upd = normed * gain_ref[...] * alive(cnt_ref, step, tile)
    high, low = split(upd)
    hot = hot_rows(receiver_place(rr_ref[...], core, rows), 2 * rows)
    agg_ref[...] += mm(hot, high) + mm(hot, low)


def node_both(
    g_ref, near_ref, far_ref, agg_ref, got_ref, cot_ref, cot_far_ref, w1_ref, w2_ref, gain_ref,
    gin_ref, gagg_ref, gw_ref, acts,
):
    rows = cot_ref.shape[0]
    width = cot_ref.shape[1]
    g = g_ref[CORE]
    nodes = jnp.concatenate([near_ref[...], far_ref[...]], axis=0)
    agg = jnp.concatenate(
        [agg_ref[:rows] + got_ref[rows:], agg_ref[rows:] + got_ref[:rows]], axis=0
    ).astype(BF)
    cot = jnp.concatenate([cot_ref[...], cot_far_ref[...]], axis=0)
    pre = mm(nodes, w1_ref[:width]) + mm(agg, w1_ref[width:])
    sig = sigmoid(pre)
    act = (pre * sig).astype(BF)
    acts[...] = act
    normed, inv_std = norm_forward(mm(act, w2_ref[...]))
    gout = norm_backward(cot, gain_ref[...], normed, inv_std).astype(BF)
    gpre = (mm_nt(gout, w2_ref[...]) * (sig * (1.0 + pre * (1.0 - sig)))).astype(BF)
    gin_ref[...] = cot_ref[...] + mm_nt(gpre[:rows], w1_ref[:width])
    gagg_ref[...] = mm_nt(gpre, w1_ref[width:])
    part = jnp.where(g == 0, nodes.astype(F32), agg.astype(F32)).astype(BF)
    gw_ref[:width] = mm_tn(part, gpre).astype(BF)
    some = acts[:, pl.ds(pl.multiple_of(g * (width // 2), 128), width // 2)]
    gw_ref[width:] = mm_tn(some, gout).astype(BF)


def edge_backward(
    cnt_ref, g_ref, cot_ref, gagg_ref, rc_ref, pre_ref, out_ref, low_ref, ein_ref, w2_ref, gain_ref, node_ref,
    gpre_ref, mine_ref, theirs_ref, high, rest, acts, gouts, eins,
):
    step = pl.program_id(0)
    tile, width = cot_ref.shape

    @pl.when(step == 0)
    def _():
        a, b = split(gagg_ref[...])
        high[...] = a
        rest[...] = b

    rows = gagg_ref.shape[0] // 2
    hot = hot_cols(receiver_place(rc_ref[...], g_ref[CORE], rows), 2 * rows)
    grad = cot_ref[...] + (mm(hot, high[...]) + mm(hot, rest[...]))
    grad = grad * alive(cnt_ref, step, tile)
    normed, inv_std = norm_forward(out_ref[...])
    gout = norm_backward(grad, gain_ref[...], normed, inv_std).astype(BF)
    pre = pre_ref[...]
    sig = sigmoid(pre)
    here = pl.ds(pl.multiple_of(step * tile, tile), tile)
    acts[here] = (pre * sig).astype(BF)
    gouts[here] = gout
    eins[here, :width] = low_ref[...]
    eins[here, width:] = ein_ref[...]
    gpre_ref[here] = (mm_nt(gout, w2_ref[...]) * (sig * (1.0 + pre * (1.0 - sig)))).astype(BF)

    @pl.when(step == pl.num_programs(0) - 1)
    def _():
        big, small = 3 * width // 2, width // 2
        mine_ref[2 * width :] = node_ref[...]
        for k in range(2):
            side = g_ref[CORE] if k == 1 else 1 - g_ref[CORE]
            cols = eins[:, pl.ds(pl.multiple_of(side * big, 128), big)]
            some = acts[:, pl.ds(pl.multiple_of(side * small, 128), small)]
            first = mm_tn(cols, gpre_ref[...])
            second = mm_tn(some, gouts[...])
            dst = mine_ref if k == 1 else theirs_ref
            dst[:big] = first.astype(dst.dtype)
            dst[big : big + small] = second.astype(dst.dtype)


def edge_inputs(
    g_ref, gpre_ref, cot_ref, sr_ref, rr_ref, w1_ref, grad_ref, mine_ref, theirs_ref, sent, recvd,
):
    step = pl.program_id(0)
    width = cot_ref.shape[1]
    half, rows = sent.shape[0] // 2, recvd.shape[0] // 2

    @pl.when(step == 0)
    def _():
        sent[...] = jnp.zeros_like(sent)
        recvd[...] = jnp.zeros_like(recvd)

    gpre = gpre_ref[...]
    grad_ref[...] = cot_ref[...] + mm_nt(gpre, w1_ref[...])
    core = g_ref[CORE]
    sent[...] += mm(hot_rows(sender_place(sr_ref[...], core, rows), 2 * half), gpre)
    recvd[...] += mm(hot_rows(receiver_place(rr_ref[...], core, rows), 2 * rows), gpre)

    @pl.when(step == pl.num_programs(0) - 1)
    def _():
        mine_ref[:half] = sent[:half]
        mine_ref[half:] = recvd[:rows]
        theirs_ref[:half] = sent[half:].astype(BF)
        theirs_ref[half:] = recvd[rows:].astype(BF)


def whole(shape):
    return pl.BlockSpec(shape, lambda i: (0,) * len(shape))


def rows_of(tile, width):
    return pl.BlockSpec((tile, width), lambda i: (i, 0))


def cols_of(tile):
    return pl.BlockSpec((1, tile), lambda i: (0, i))


SMEM = pl.BlockSpec(memory_space=pltpu.SMEM)


def call(body, grid, ins, outs, shapes, scratch, flops, traffic, limit):
    return pl.pallas_call(
        body,
        grid=(grid,),
        in_specs=ins,
        out_specs=outs,
        out_shape=[jax.ShapeDtypeStruct(s, d) for s, d in shapes],
        scratch_shapes=[pltpu.VMEM(s, d) for s, d in scratch],
        cost_estimate=pl.CostEstimate(flops=flops, bytes_accessed=traffic, transcendentals=0),
        compiler_params=pltpu.CompilerParams(
            dimension_semantics=("arbitrary",), vmem_limit_bytes=limit << 20
        ),
    )


def node_finish(mine_ref, got_ref, next_ref, prev_ref, gin_ref, ws_ref, wr_ref, out_ref):
    rows = gin_ref.shape[0]
    mid = slice(rows, 2 * rows)
    sent = mine_ref[mid] + got_ref[mid].astype(F32)
    sent = (sent + next_ref[...].astype(F32) + prev_ref[...].astype(F32)).astype(BF)
    recvd = (mine_ref[3 * rows :] + got_ref[3 * rows :].astype(F32)).astype(BF)
    out_ref[...] = (
        gin_ref[...]
        + mm_nt(sent, ws_ref[...])
        + mm_nt(recvd, wr_ref[...])
    )


def pack(slot_ref, mine_ref, far_ref, own_ref, *refs):
    sends, last = refs[:-1], refs[-1]
    count = mine_ref.shape[0] // own_ref.shape[0]
    edge = far_ref.shape[0]
    node = mine_ref.shape[0] - edge
    for j, dst in enumerate((own_ref, *sends[:-2], last)):
        rows, base = 0, 0
        for whole_size in (3 * edge // 4, edge // 4, 2 * node // 3, node // 3):
            size = whole_size // count
            here = pl.ds(pl.multiple_of(base + slot_ref[j] * size, 32), size)
            value = mine_ref[here]
            if base < edge:
                value = (value.astype(F32) + far_ref[here].astype(F32)).astype(BF)
            dst[rows : rows + size] = value
            rows += size
            base += whole_size
    middle = last.shape[0] // 2
    sends[-2][...] = last[:middle]
    sends[-1][...] = last[middle:]


def merge(_, up_ref, down_ref, first_ref, second_ref, up_out, down_out):
    middle = first_ref.shape[0]
    up_out[:middle] = (up_ref[:middle].astype(F32) + first_ref[...].astype(F32)).astype(BF)
    up_out[middle:] = up_ref[middle:]
    down_out[:middle] = down_ref[:middle]
    down_out[middle:] = (down_ref[middle:].astype(F32) + second_ref[...].astype(F32)).astype(BF)


def unpack(slot_ref, *refs):
    *parts, half_ref, rest_ref, first_ref, second_ref, third_ref, fourth_ref, last = refs
    middle = half_ref.shape[0]
    last[:middle] = half_ref[...]
    last[middle:] = rest_ref[...]
    parts.append(last)
    count = len(parts)
    for j, part in enumerate(parts):
        rows = 0
        for dst in (first_ref, second_ref, third_ref, fourth_ref):
            size = dst.shape[0] // count
            here = pl.ds(pl.multiple_of(slot_ref[j] * size, 32), size)
            dst[here] = part[rows : rows + size].astype(F32)
            rows += size


def sum_and_split(count, slot_ref, own_ref, *refs):
    got, total, sends = refs[:count], refs[-1], refs[count:-1]
    value = own_ref[...].astype(F32)
    for part in got:
        value = value + part[...].astype(F32)
    total[...] = value
    size = sends[0].shape[0]
    for j, dst in enumerate(sends):
        here = pl.ds(pl.multiple_of(slot_ref[j] * size, 8), size)
        dst[...] = total[here].astype(dst.dtype)


def join(slot_ref, *refs):
    parts, dst = refs[:-1], refs[-1]
    size = parts[0].shape[0]
    for j, part in enumerate(parts):
        here = pl.ds(pl.multiple_of(slot_ref[j] * size, 8), size)
        dst[here] = part[...].astype(dst.dtype)


class From:
    def __init__(self, ref, base):
        self.ref, self.base = ref, base

    def __getitem__(self, j):
        return self.ref[self.base + j]


def small_call(body, base, args, shapes, scratch):
    def run(table_ref, *refs):
        body(From(table_ref, base), *refs)

    return call(
        run, 1, [SMEM] + [whole(a.shape) for a in args[1:]], [whole(s) for s, _ in shapes],
        shapes, scratch, 1 << 20, sum(int(np.prod(s)) * 4 for s, _ in shapes), 12,
    )(*args)


def scalars(sizes, steps):
    _, ny, nx = sizes
    where, g = lax.axis_index("patch"), lax.axis_index("grp")
    x, y, z = lax.rem(where, nx), lax.rem(lax.div(where, nx), ny), lax.div(where, nx * ny)
    moves = [0] + steps
    offsets = np.array(moves + moves + [-s for s in moves] * 2 + [0, 1, 0], np.int32)
    kind = np.array([0] * 4 + [1] * 4 + [1] * 4 + [0] * 4 + [2, 2, 3], np.int32)
    first, second = jnp.where(g == 0, x, y), jnp.where(g == 0, y, x)
    bit = jnp.bitwise_and(jnp.bitwise_xor(lax.div(z, 2), z), 1)
    slot = lax.rem(jnp.where(kind == 0, first, second) + offsets + nx, nx)
    half = jnp.bitwise_xor(bit, offsets)
    return jnp.where(kind == 3, g, jnp.where(kind == 2, half, slot)).astype(jnp.int32)


def sum_over_patches(mine, far, sizes, steps, table, others):
    nz, ny, nx = sizes
    n = nx
    width = mine.shape[1]

    def send(value, move):
        pairs = []
        for source in range(2 * nz * ny * nx):
            to = move(*[int(v) for v in np.unravel_index(source, (nz, ny, nx, 2))])
            pairs.append((source, int(np.ravel_multi_index(to, (nz, ny, nx, 2)))))
        return lax.ppermute(value, ("patch", "grp"), pairs)

    def shift(value, leg, s):
        def move(z, y, x, g):
            return (z, y, (x + s) % nx, g) if g == leg else (z, (y + s) % ny, x, g)

        return send(value, move)

    def flip(value, partner):
        return send(value, lambda z, y, x, g: (partner[z], y, x, g))

    rows = mine.shape[0] // n
    own, up, down, half, rest = small_call(
        pack, 0, (table, mine, far),
        [((rows, width), BF)] * 3 + [((rows // 2, width), BF)] * 2, [((rows, width), BF)],
    )
    up, down = small_call(
        merge, 0, (table, up, down, shift(half, 0, 1), shift(rest, 0, -1)),
        [((rows, width), BF)] * 2, [],
    )
    got = [shift(up, 0, 1), shift(down, 0, -1)]
    inputs = others.inputs()
    own, *out = small_call(
        functools.partial(sum_and_split, 2), 4, (table, own, *got),
        [((rows // n, width), F32)] + [((rows // n, width), BF)] * (n - 1),
        [((rows, width), F32)],
    )
    got = [shift(v, 1, s) for v, s in zip(out, steps)]
    sums = others.swap(inputs)
    rows //= n
    near = [k ^ 1 for k in range(nz)]
    next_to = [(k + 1) % nz if k % 2 else (k - 1) % nz for k in range(nz)]
    across = [(k // 4) * 4 + 3 - k % 4 if k % 4 in (0, 3) else nz - 1 - k for k in range(nz)]
    keep, out = small_call(
        functools.partial(sum_and_split, n - 1), 16, (table, own, *got),
        [((rows // 2, width), F32), ((rows // 2, width), BF)],
        [((rows, width), F32)],
    )
    part = (keep + flip(out, near).astype(F32)).astype(BF)
    sums = others.shift(sums)
    part = (part.astype(F32) + flip(part, next_to).astype(F32)).astype(BF)
    part = (part.astype(F32) + flip(part, across).astype(F32)).astype(BF)
    node_grad = others.finish(sums)
    (part,) = small_call(join, 16, (table, part, flip(part, near)), [((rows, width), BF)], [])
    (part,) = small_call(
        join, 8, (table, part, *[shift(part, 1, s) for s in steps]),
        [((rows * n, width), BF)], [],
    )
    tall = far.shape[0] // 4
    short = (mine.shape[0] - far.shape[0]) // 3
    before, behind = shift(part, 0, 1), shift(part, 0, -1)
    middle = before.shape[0] // 2
    weights = small_call(
        unpack, 12, (table, part, before, behind, shift(before[:middle], 0, 1), shift(behind[middle:], 0, -1)),
        [((3 * tall, width), F32), ((tall, width), F32), ((2 * short, width), F32), ((short, width), F32)],
        [((rows * n, width), BF)],
    )
    return node_grad, inputs[0], *weights


class Others:
    def __init__(self, inputs, swap, shift, finish):
        self.inputs, self.swap, self.shift, self.finish = inputs, swap, shift, finish


def local(
    node_latent, edge_latent, node_cot, edge_cot, edge_w1, edge_w2, edge_gain,
    node_w1, node_w2, node_gain, senders, receivers, counts,
):
    rows, width = node_latent.shape
    edges = edge_latent.shape[0]
    tiles = edges // TILE
    n_patch = lax.axis_size("patch")
    other = [(0, 1), (1, 0)]
    up = [(i, (i + 1) % n_patch) for i in range(n_patch)]
    down = [(j, i) for i, j in up]

    node_bf = node_latent.astype(BF)
    sizes = (n_patch // 16, 4, 4)
    steps = [1, -1, 2]
    table = scalars(sizes, steps)

    def fetch(step, cross):
        pairs = [
            (2 * p + c, 2 * ((p - step) % n_patch) + (c ^ cross)) for p in range(n_patch) for c in (0, 1)
        ]
        return lax.ppermute(node_bf, ("patch", "grp"), pairs)

    near = [fetch(-1, 0), node_bf, fetch(1, 0)]
    far = [fetch(-1, 1), fetch(0, 1), fetch(1, 1)]
    cot_far = lax.ppermute(node_cot, "grp", other)

    send_col, send_row = senders[:, None], senders[None, :]
    recv_col, recv_row = receivers[:, None], receivers[None, :]
    egain, ngain = edge_gain[None, :], node_gain[None, :]

    sq = edges * width * width
    edge_low, edge_part = call(
        edge_first, tiles,
        [SMEM, rows_of(TILE, width), pl.BlockSpec((width, width), lambda i: (0, 0))],
        [rows_of(TILE, width), rows_of(TILE, width)],
        [((edges, width), BF), ((edges, width), F32)],
        [], 2 * sq, 5 << 20, 12,
    )(table, edge_latent, edge_w1)
    edge_in, edge_pre, edge_out, agg = call(
        edge_forward, tiles,
        [SMEM, SMEM, rows_of(TILE, width)] + [whole((rows, width))] * 6
        + [rows_of(TILE, 1), rows_of(TILE, 1), cols_of(TILE),
           pl.BlockSpec((width, width), lambda i: (1, 0)), pl.BlockSpec((width, width), lambda i: (2, 0)),
           whole((width, width)), whole((1, width))],
        [rows_of(TILE, 2 * width), rows_of(TILE, width), rows_of(TILE, width), whole((2 * rows, width))],
        [((edges, 2 * width), BF), ((edges, width), F32), ((edges, width), F32), ((2 * rows, width), F32)],
        [((6 * rows, width), BF), ((2 * rows, width), BF)],
        12 * sq, 12 << 20, 20,
    )(counts, table, edge_part, *near, *far, send_col, recv_col, recv_row, edge_w1, edge_w1, edge_w2, egain)

    agg_far = lax.ppermute(agg, "grp", other)
    node_gin, gagg, node_gw = call(
        node_both, 1,
        [SMEM, whole((rows, width)), whole((rows, width)), whole((2 * rows, width)),
         whole((2 * rows, width)), whole((rows, width)), whole((rows, width)),
         whole((2 * width, width)), whole((width, width)), whole((1, width))],
        [whole((rows, width)), whole((2 * rows, width)), whole((3 * width // 2, width))],
        [((rows, width), F32), ((2 * rows, width), F32), ((3 * width // 2, width), BF)],
        [((2 * rows, width), BF)],
        5 * sq, 6 << 20, 20,
    )(table, near[1], far[1], agg, agg_far, node_cot, cot_far, node_w1, node_w2, ngain)

    gpre, gw_mine, gw_theirs = call(
        edge_backward, tiles,
        [SMEM, SMEM, rows_of(TILE, width), whole((2 * rows, width)), rows_of(TILE, 1),
         rows_of(TILE, width), rows_of(TILE, width), rows_of(TILE, width), rows_of(TILE, 2 * width),
         whole((width, width)), whole((1, width)),
         whole((3 * width // 2, width))],
        [whole((edges, width)), whole((7 * width // 2, width)), whole((2 * width, width))],
        [((edges, width), BF), ((7 * width // 2, width), BF), ((2 * width, width), BF)],
        [((2 * rows, width), BF), ((2 * rows, width), BF), ((edges, width), BF), ((edges, width), BF),
         ((edges, 3 * width), BF)],
        12 * sq, 14 << 20, 20,
    )(counts, table, edge_cot, gagg, recv_col, edge_pre, edge_out, edge_low, edge_in, edge_w2, egain, node_gw)

    gw_far = lax.ppermute(gw_theirs, "grp", other)

    def inputs():
        return call(
            edge_inputs, tiles,
            [SMEM, rows_of(TILE, width), rows_of(TILE, width), cols_of(TILE), cols_of(TILE),
             whole((width, width))],
            [rows_of(TILE, width), whole((4 * rows, width)), whole((4 * rows, width))],
            [((edges, width), F32), ((4 * rows, width), F32), ((4 * rows, width), BF)],
            [((6 * rows, width), F32), ((2 * rows, width), F32)],
            8 * sq, 6 << 20, 16,
        )(table, gpre, edge_cot, send_row, recv_row, edge_w1)

    def swap(made):
        return made[1], lax.ppermute(made[2], "grp", other)

    def shift(sums):
        mine, far = sums
        ends = [
            (mine[at : at + rows] + far[at : at + rows].astype(F32)).astype(BF) for at in (0, 2 * rows)
        ]
        return (
            mine, far,
            lax.ppermute(ends[0], "patch", down),
            lax.ppermute(ends[1], "patch", up),
        )

    def finish(sums):
        return call(
            node_finish, 1,
            [whole((4 * rows, width)), whole((4 * rows, width)), whole((rows, width)),
             whole((rows, width)), whole((rows, width)),
             pl.BlockSpec((width, width), lambda i: (1, 0)), pl.BlockSpec((width, width), lambda i: (2, 0))],
            [whole((rows, width))],
            [((rows, width), F32)],
            [],
            sq // 2, 2 << 20, 16,
        )(*sums, node_gin, edge_w1, edge_w1)[0]

    return sum_over_patches(
        gw_mine, gw_far, sizes, steps, table, Others(inputs, swap, shift, finish)
    )


def solution(mesh):
    split_rows = P(("patch", "grp"), None)
    flat = P(("patch", "grp"))
    in_specs = (split_rows,) * 4 + (P(),) * 6 + (flat,) * 3
    out_specs = (split_rows, split_rows) + (P("grp", None),) * 4

    return jax.shard_map(local, mesh=mesh, in_specs=in_specs, out_specs=out_specs, check_vma=False)
```
